32 devices in a mesh: row: 4 (over z), col: 8 (over y, x, core).
Axes of the slice: x: 2, y: 2, z: 4, core: 2. Of those that a mesh axis runs over, the one named last changes fastest.
Arguments:
- tokens: bfloat16 [512, 12288], P('row', 'col'), may hold values from -6 to 6
- prev_tokens: bfloat16 [512, 12288], P('row', 'col'), may hold values from -6 to 6
- hidden_grad: bfloat16 [512, 49152], P('col', 'row'), may hold values from -6 to 6
- active_blocks: int32 [1], replicated, may hold values from 6 to 16
- weight: bfloat16 [12288, 49152], P('col', 'row'), may hold values from -0.0546875 to 0.0546875
Outputs:
- activation: bfloat16 [512, 49152], P('col', 'row')
- weight_grad: bfloat16 [12288, 49152], P('col', 'row')
The draws below stay inside these ranges and needn't reach their ends.
Inputs may be any that keep to these rules, and one draw needn't show every extreme that they name: The sampled blocks are the first active_blocks[0] blocks of 3072 hidden units.
All inputs are finite; a program needn't handle non-finite values.
Results may differ from the reference program's by a relative error of at most 0.001.
Values may be sent and summed in bfloat16 or wider, within the bound.
A program may use at most 640 MiB of HBM per device.

```python
import jax
import jax.numpy as jnp
from jax import lax

D = 12288
FF = 49152
BLOCK = 3072
TOKENS = 512
DSLAB = 1536
N_COL = 8


def shard_levels(stream_key, extent, shards, least, largest):
    def one(dim, blocks):
        steps = jax.random.uniform(jax.random.fold_in(jax.random.fold_in(stream_key, 6), dim), (blocks,), jnp.float32, least / len(shards), largest / len(shards))
        return jnp.repeat(jnp.exp(steps), extent[dim] // blocks).reshape((-1,) + (1,) * (len(extent) - dim - 1))

    loudness = one(*shards[0])
    for cut in shards[1:]:
        loudness = loudness * one(*cut)
    return loudness


def gaussian(own_key, extent, spread, bound, pieces=(), held_as=jnp.bfloat16):
    array = jax.random.normal(own_key, extent, jnp.float32) * spread
    if len(pieces) > 0:
        array = shard_levels(own_key, extent, pieces, -0.22, 0.18) * array
    return jnp.clip(array, min=-bound, max=bound).astype(held_as)


def setup_inputs(seed: int = 0) -> dict:
    seeds = jax.random.split(jax.random.key(seed), 6)
    return {
        "tokens": gaussian(seeds[0], (TOKENS, D), 1.0, 6.0, ((0, 4), (1, 8))),
        "prev_tokens": gaussian(seeds[1], (TOKENS, D), 1.0, 6.0, ((0, 4), (1, 8))),
        "hidden_grad": gaussian(seeds[2], (TOKENS, FF), 1.0, 6.0, ((0, 8), (1, 4))),
        "active_blocks": jax.random.randint(seeds[3], (1,), 6, 17).astype(jnp.int32),
        "weight": gaussian(seeds[4], (D, FF), D ** -0.5, 0.0546875, ((0, 8), (1, 4))),
    }


def reference(tokens, prev_tokens, hidden_grad, active_blocks, weight):
    unit_limit = active_blocks[0] * BLOCK
    unit_mask = (jnp.arange(FF, dtype=jnp.int32) < unit_limit).astype(jnp.float32)

    def add_slab(running, index):
        columns = lax.dynamic_slice_in_dim(tokens, (index * DSLAB).astype(jnp.int32), DSLAB, 1)
        weight_rows = lax.dynamic_slice_in_dim(weight, (index * DSLAB).astype(jnp.int32), DSLAB, 0)
        partial_value = jnp.dot(columns, weight_rows, preferred_element_type=jnp.float32)
        return running + partial_value, None

    hidden, unused = lax.scan(add_slab, jnp.zeros((TOKENS, FF), jnp.float32), jnp.arange(N_COL, dtype=jnp.int32))
    activation = (jax.nn.gelu(hidden, approximate=False) * unit_mask).astype(jnp.bfloat16)

    def grad_block(index):
        offset = (index * BLOCK).astype(jnp.int32)
        grad_cols = lax.dynamic_slice_in_dim(hidden_grad, offset, BLOCK, 1)
        mask_cols = lax.dynamic_slice_in_dim(unit_mask, offset, BLOCK, 0)
        block_grad = lax.dot_general(prev_tokens, grad_cols, (((0,), (0,)), ((), ())), preferred_element_type=jnp.float32)
        return (block_grad * mask_cols).astype(jnp.bfloat16)

    blocks = lax.map(grad_block, jnp.arange(FF // BLOCK, dtype=jnp.int32))
    weight_grad = jnp.transpose(blocks, (1, 0, 2)).reshape(D, FF)
    return activation, weight_grad
```

```python
import jax
import jax.numpy as jnp
from jax import lax
from jax.sharding import PartitionSpec as P

BLOCK = 3072
TOKEN_BOUND = 6.0
WEIGHT_BOUND = 0.0546875


def exchange(value, bit):
    size = lax.axis_size("col")
    return lax.ppermute(value, "col", [(i, i ^ bit) for i in range(size)])


def shift(value, step):
    size = lax.axis_size("row")
    return lax.ppermute(value, "row", [(i, (i + step) % size) for i in range(size)])


def gather_rows(block):
    size = lax.axis_size("row")
    half = size // 2
    found = {0: block}
    up, down = block, block
    for distance in range(1, half):
        up, down = shift(up, 1), shift(down, -1)
        found[distance], found[size - distance] = up, down
    cut = block.shape[0] // 2
    found[half] = jnp.concatenate([shift(up[:cut], 1), shift(down[cut:], -1)], axis=0)
    return jnp.concatenate([found[d] for d in range(size)], axis=0), found[half]


def rows_of(ring, owners, count, per_row):
    size = lax.axis_size("row")
    above = lax.axis_index("row").astype(jnp.uint32) + jnp.uint32(size)
    zero = jnp.uint32(0)
    pieces = []
    for owner in owners:
        first = owner * jnp.uint32(count)
        away = lax.rem(above - lax.div(first, jnp.uint32(per_row)), jnp.uint32(size))
        start = away * jnp.uint32(per_row) + lax.rem(first, jnp.uint32(per_row))
        pieces.append(lax.dynamic_slice(ring, (start, zero), (count, ring.shape[1])))
    return jnp.concatenate(pieces, axis=0)


def shards(tokens, prev_tokens, hidden_grad, active_blocks, weight):
    local_units = weight.shape[1]
    size = lax.axis_size("col")
    me = lax.axis_index("col").astype(jnp.uint32)
    per_row = tokens.shape[0]
    count = hidden_grad.shape[0]
    part_rows = count // 2
    chip_bits = []
    bit = 2
    while bit < size:
        chip_bits.append(bit)
        bit *= 2
    orders = (chip_bits, chip_bits[::-1])
    chip_masks = list(range(0, size, 2))

    first_unit = lax.axis_index("row") * local_units
    unit_limit = active_blocks[0] * BLOCK
    unit_ids = first_unit + lax.iota(jnp.int32, local_units)
    unit_mask = (unit_ids < unit_limit).astype(jnp.float32)

    grads = {}
    for part, order in enumerate(orders):
        held = {0: hidden_grad[part * part_rows : (part + 1) * part_rows]}
        for bit in order:
            held.update({m ^ bit: exchange(piece, bit) for m, piece in list(held.items())})
        held.update({m ^ 1: exchange(piece, 1) for m, piece in list(held.items())})
        grads.update({(m, part): piece for m, piece in held.items()})

    ring, last = gather_rows(tokens)
    far = rows_of(ring, [me ^ jnp.uint32(m ^ 1) for m in chip_masks], count, per_row)
    near = rows_of(ring, [me ^ jnp.uint32(m) for m in chip_masks], count, per_row)
    depth = weight.shape[0] * size
    scale = 1.0
    while scale * 2.0 * depth * TOKEN_BOUND * WEIGHT_BOUND < 65504.0:
        scale *= 2.0

    def narrow(value):
        return (value * scale).astype(jnp.float16)

    def widen(value):
        return value.astype(jnp.float32) * (1.0 / scale)

    for_partner = narrow(jnp.dot(far, weight, preferred_element_type=jnp.float32))
    from_partner = exchange(for_partner, 1)
    chip_sum = jnp.dot(near, weight, preferred_element_type=jnp.float32) + widen(from_partner)
    chip_sum = chip_sum.reshape(len(chip_masks), 2, part_rows, local_units)
    parts = []
    for part, order in enumerate(orders):
        held = {m: chip_sum[i, part] for i, m in enumerate(chip_masks)}
        for bit in order:
            for m in sorted((m for m in held if m & bit), reverse=True):
                value = held.pop(m)
                got = exchange(value, bit) if bit == order[-1] else widen(exchange(narrow(value), bit))
                held[m ^ bit] = held[m ^ bit] + got
        parts.append(held[0])
    hidden = jnp.concatenate(parts, axis=0)
    activation = (jax.nn.gelu(hidden, approximate=False) * unit_mask).astype(jnp.bfloat16)

    earlier_ring, last = gather_rows(prev_tokens + last[:1, :1] * 0)
    earlier = rows_of(earlier_ring, [me ^ jnp.uint32(m) for m in range(size)], count, per_row)
    grad_rows = jnp.concatenate([grads[m, part] for m in range(size) for part in range(2)], axis=0)
    grad_sum = lax.dot_general(
        earlier, grad_rows, (((0,), (0,)), ((), ())), preferred_element_type=jnp.float32
    )
    weight_grad = (grad_sum * unit_mask).astype(jnp.bfloat16)
    return (activation, weight_grad)


def solution(mesh):
    return jax.shard_map(
        shards,
        mesh=mesh,
        in_specs=(P("row", "col"), P("row", "col"), P("col", "row"), P(), P("col", "row")),
        out_specs=(P("col", "row"), P("col", "row")),
        check_vma=False,
    )
```

```python
import jax
import jax.numpy as jnp
from jax import lax
from jax.sharding import PartitionSpec as P

BLOCK = 3072
TOKEN_BOUND = 6.0
WEIGHT_BOUND = 0.0546875


def exchange(value, bit):
    size = lax.axis_size("col")
    return lax.ppermute(value, "col", [(i, i ^ bit) for i in range(size)])


def shift(value, step):
    size = lax.axis_size("row")
    return lax.ppermute(value, "row", [(i, (i + step) % size) for i in range(size)])


def gather_rows(block):
    size = lax.axis_size("row")
    half = size // 2
    found = {0: block}
    up, down = block, block
    for distance in range(1, half):
        up, down = shift(up, 1), shift(down, -1)
        found[distance], found[size - distance] = up, down
    cut = block.shape[0] // 2
    found[half] = jnp.concatenate([shift(up[:cut], 1), shift(down[cut:], -1)], axis=0)
    return jnp.concatenate([found[d] for d in range(size)], axis=0)


def rows_of(ring, owners, count, per_row):
    size = lax.axis_size("row")
    above = lax.axis_index("row").astype(jnp.uint32) + jnp.uint32(size)
    zero = jnp.uint32(0)
    pieces = []
    for owner in owners:
        first = owner * jnp.uint32(count)
        away = lax.rem(above - lax.div(first, jnp.uint32(per_row)), jnp.uint32(size))
        start = away * jnp.uint32(per_row) + lax.rem(first, jnp.uint32(per_row))
        pieces.append(lax.dynamic_slice(ring, (start, zero), (count, ring.shape[1])))
    return jnp.concatenate(pieces, axis=0)


def shards(tokens, prev_tokens, hidden_grad, active_blocks, weight):
    local_units = weight.shape[1]
    size = lax.axis_size("col")
    me = lax.axis_index("col").astype(jnp.uint32)
    per_row = tokens.shape[0]
    count = hidden_grad.shape[0]
    part_rows = count // 2
    chip_bits = []
    bit = 2
    while bit < size:
        chip_bits.append(bit)
        bit *= 2
    orders = (chip_bits, chip_bits[::-1])
    chip_masks = list(range(0, size, 2))

    first_unit = lax.axis_index("row") * local_units
    unit_limit = active_blocks[0] * BLOCK
    unit_ids = first_unit + lax.iota(jnp.int32, local_units)
    unit_mask = (unit_ids < unit_limit).astype(jnp.float32)

    grads = {}
    for part, order in enumerate(orders):
        held = {0: hidden_grad[part * part_rows : (part + 1) * part_rows]}
        for bit in order:
            held.update({m ^ bit: exchange(piece, bit) for m, piece in list(held.items())})
        held.update({m ^ 1: exchange(piece, 1) for m, piece in list(held.items())})
        grads.update({(m, part): piece for m, piece in held.items()})

    ring = gather_rows(tokens)
    far = rows_of(ring, [me ^ jnp.uint32(m ^ 1) for m in chip_masks], count, per_row)
    near = rows_of(ring, [me ^ jnp.uint32(m) for m in chip_masks], count, per_row)
    depth = weight.shape[0] * size
    scale = 1.0
    while scale * 2.0 * depth * TOKEN_BOUND * WEIGHT_BOUND < 65504.0:
        scale *= 2.0

    def narrow(value):
        return (value * scale).astype(jnp.float16)

    def widen(value):
        return value.astype(jnp.float32) * (1.0 / scale)

    for_partner = narrow(jnp.dot(far, weight, preferred_element_type=jnp.float32))
    from_partner = exchange(for_partner, 1)
    relayed = sum(grads[m, part][:1, :1] for part, m in enumerate((orders[0][0], orders[1][0])))
    near = near + relayed * 0
    own_sum = lax.optimization_barrier(jnp.dot(near, weight, preferred_element_type=jnp.float32))
    pair_sums = own_sum.reshape(len(chip_masks), 2, part_rows, local_units)
    pair_recv = from_partner.reshape(len(chip_masks), 2, part_rows, local_units)
    parts = [
        {m: pair_sums[i, part] + widen(pair_recv[i, part]) for i, m in enumerate(chip_masks)}
        for part in range(2)
    ]
    tie = jnp.zeros((1, 1), jnp.float32)
    after_sums = jnp.zeros((1, 1), jnp.bfloat16)
    finals = []
    for step in range(len(chip_bits)):
        arrived = []
        for held, order in zip(parts, orders):
            bit = order[step]
            sent = [m for m in sorted(held) if m & bit]
            value = jnp.concatenate([held.pop(m) for m in sent], axis=0) + tie
            last_step = step == len(chip_bits) - 1
            outgoing = value if last_step else narrow(value)
            if step == 0:
                after_sums = after_sums + (outgoing[:1, :1] * 0).astype(jnp.bfloat16)
            got = exchange(outgoing, bit) if last_step else widen(exchange(outgoing, bit))
            if last_step:
                finals.append((held[0], got))
                continue
            for i, m in enumerate(sent):
                held[m ^ bit] = held[m ^ bit] + got[i * part_rows : (i + 1) * part_rows]
            arrived.append(got[:1, :1])
        if arrived:
            tie = (arrived[0] + arrived[1]) * 0.0
    after_far = (for_partner[:1, :1] * 0).astype(prev_tokens.dtype)
    earlier_ring = gather_rows(prev_tokens + after_far)
    earlier = rows_of(earlier_ring, [me ^ jnp.uint32(m) for m in range(size)], count, per_row)
    grad_rows = jnp.concatenate(
        [grads[m, part] + after_sums if m else grads[m, part] for m in range(size) for part in range(2)],
        axis=0,
    )
    grad_sum = lax.dot_general(
        earlier, grad_rows, (((0,), (0,)), ((), ())), preferred_element_type=jnp.float32
    )
    weight_grad = (grad_sum * unit_mask).astype(jnp.bfloat16)
    after_grad = weight_grad[:1, :1].astype(jnp.float32) * 0.0
    hidden = jnp.concatenate([kept + (got + after_grad) for kept, got in finals], axis=0)
    activation = (jax.nn.gelu(hidden, approximate=False) * unit_mask).astype(jnp.bfloat16)
    return (activation, weight_grad)


def solution(mesh):
    return jax.shard_map(
        shards,
        mesh=mesh,
        in_specs=(P("row", "col"), P("row", "col"), P("col", "row"), P(), P("col", "row")),
        out_specs=(P("col", "row"), P("col", "row")),
        check_vma=False,
    )
```
